32 devices in a mesh: cuts: 2 (over x), wide: 8 (over z, y), narrow: 2 (over core).
Axes of the slice: x: 2, y: 2, z: 4, core: 2. Of those that a mesh axis runs over, the one named last changes fastest.
Arguments:
- stem_tensor: float32 [2, 16384, 512], P(None, ('cuts', 'wide', 'narrow')), parts along dimension 1, may hold values from -6 to 6
- leaves: bfloat16 [16, 4, 2, 512, 512], P(('cuts', 'wide')), parts along dimension 0, may hold values from -1 to 1
- root_devices: int32 [4], replicated, may hold values from 0 to 7, as said below
- mode_orders: int32 [4, 9], replicated, may hold values from 0 to 8, each once within a row
Outputs:
- contracted: float32 [2, 16384, 512], P(None, ('cuts', 'wide', 'narrow')), parts along dimension 1
The draws below stay inside these ranges and needn't reach their ends.
There are 2 independent parts, one for each index of `cuts`. The reference program is written for one: setup_inputs(seed, part) draws one part's arguments, and reference() takes and returns one part's arrays. A program takes and returns all parts, laid end to end along the dimension named above; an argument that names none is the same for every part. Nothing has to cross between parts.
Inputs may be any that keep to these rules, and one draw needn't show every extreme that they name: `root_devices`: the roots include 0, 4 and 7. `mode_orders`: each row holds every number of 0 to 8 once.
All inputs are finite; a program needn't handle non-finite values.
Results may differ from the reference program's by a relative error of at most 0.0081.
Values may be sent and summed in bfloat16 or wider, within the bound.
A program may use at most 64 MiB of HBM per device.

```python
import math
import jax
import jax.numpy as jnp
from jax import lax

MODES = 9
BRANCH = 512
ROWS_DEV = 512
STEPS = 4
ROWS = 8192
N_WIDE = 8
N_NARROW = 2


def draw_root_devices(key, part):
    order = jax.random.permutation(jax.random.fold_in(key, 11), STEPS)
    extra = jax.random.randint(jax.random.fold_in(key, 12), (STEPS,), 0, N_WIDE, dtype=jnp.int32)
    position = jnp.arange(STEPS, dtype=jnp.int32)
    fixed_roots = jnp.where(position == 0, 0, jnp.where(position == 1, N_WIDE // 2, N_WIDE - 1)).astype(jnp.int32)
    chosen = jnp.where(position < 3, fixed_roots, extra).astype(jnp.int32)
    return chosen[order].astype(jnp.int32)


def phase_pair(key, count):
    angles = jax.random.uniform(key, (count,), jnp.float32, -math.pi, math.pi)
    return (jnp.cos(angles), jnp.sin(angles))


def unitary_leaf(key):
    count = BRANCH
    index = jnp.arange(count, dtype=jnp.int32)
    table = index[:, None] * index[None, :] % count
    angle = table.astype(jnp.float32) * (2.0 * math.pi / count)
    scale = 1.0 / math.sqrt(count)
    fourier_re = jnp.cos(angle) * scale
    fourier_im = -jnp.sin(angle) * scale
    first_re, first_im = phase_pair(jax.random.fold_in(key, 1), count)
    middle_re, middle_im = phase_pair(jax.random.fold_in(key, 2), count)
    last_re, last_im = phase_pair(jax.random.fold_in(key, 3), count)
    shuffle = jax.random.permutation(jax.random.fold_in(key, 4), count)
    right_re = fourier_re * last_re[None, :] - fourier_im * last_im[None, :]
    right_im = fourier_re * last_im[None, :] + fourier_im * last_re[None, :]
    right_re = right_re[shuffle]
    right_im = right_im[shuffle]
    moved_re = middle_re[:, None] * right_re - middle_im[:, None] * right_im
    moved_im = middle_re[:, None] * right_im + middle_im[:, None] * right_re
    highest = lax.Precision.HIGHEST
    product_re = jnp.dot(fourier_re, moved_re, precision=highest) - jnp.dot(fourier_im, moved_im, precision=highest)
    product_im = jnp.dot(fourier_re, moved_im, precision=highest) + jnp.dot(fourier_im, moved_re, precision=highest)
    final_re = first_re[:, None] * product_re - first_im[:, None] * product_im
    final_im = first_re[:, None] * product_im + first_im[:, None] * product_re
    return jnp.clip(jnp.stack([final_re, final_im]), -1.0, 1.0)


def draw_leaves(key, part):
    keys = jax.random.split(jax.random.fold_in(key, 21), N_WIDE * STEPS)
    matrices = lax.map(unitary_leaf, keys)
    return matrices.reshape(N_WIDE, STEPS, 2, BRANCH, BRANCH).astype(jnp.bfloat16)


def shard_levels(key, dims, cuts, least, top_value):
    def one(dim, parts):
        draws = jax.random.uniform(jax.random.fold_in(jax.random.fold_in(key, 6), dim), (parts,), jnp.float32, least / len(cuts), top_value / len(cuts))
        return jnp.repeat(jnp.exp(draws), dims[dim] // parts).reshape((-1,) + (1,) * (len(dims) - dim - 1))

    loudness = one(*cuts[0])
    for cut in cuts[1:]:
        loudness = loudness * one(*cut)
    return loudness


def scatter_about(own_key, extent, width, most, cuts=(), held_as=jnp.bfloat16):
    array = width * jax.random.normal(own_key, extent, jnp.float32)
    if cuts:
        array = array * shard_levels(own_key, extent, cuts, -0.22, 0.18)
    return jnp.clip(array, -most, most).astype(held_as)


def setup_inputs(seed: int = 0, part: int = 0) -> dict:
    key_of = jax.random.split(jax.random.key(seed), 5)
    own_keys = jax.random.split(jax.random.fold_in(key_of[4], part), 5)
    stem_tensor = scatter_about(own_keys[0], (2, ROWS, BRANCH), 1.0, 6.0, ((1, 16),), jnp.float32)
    leaves = draw_leaves(jax.random.fold_in(jax.random.fold_in(key_of[4], part), 71), part)
    root_devices = draw_root_devices(jax.random.fold_in(key_of[4], 71), part)
    mode_orders = jax.vmap(lambda own: jax.random.permutation(own, MODES))(jax.random.split(key_of[3], STEPS)).reshape((STEPS, MODES)).astype(jnp.int32)
    return {"stem_tensor": stem_tensor, "leaves": leaves, "root_devices": root_devices, "mode_orders": mode_orders}


def complex_product(left_matrix, right_matrix, precision=None):
    real_part = jnp.dot(left_matrix[0], right_matrix[0], preferred_element_type=jnp.float32, precision=precision) - jnp.dot(left_matrix[1], right_matrix[1], preferred_element_type=jnp.float32, precision=precision)
    imag_part = jnp.dot(left_matrix[0], right_matrix[1], preferred_element_type=jnp.float32, precision=precision) + jnp.dot(left_matrix[1], right_matrix[0], preferred_element_type=jnp.float32, precision=precision)
    return jnp.stack([real_part, imag_part])


def column_source(order_row, branch_width):
    column = jnp.arange(branch_width, dtype=jnp.int32)
    mode_count = order_row.shape[0]
    powers = jnp.left_shift(jnp.int32(1), jnp.arange(mode_count, dtype=jnp.int32))
    bit_table = (column[:, None] // powers[None, :]) % 2
    weights = jnp.left_shift(jnp.int32(1), order_row.astype(jnp.int32))
    return jnp.sum(bit_table * weights[None, :], axis=1).astype(jnp.int32)


def reference(stem_tensor, leaves, root_devices, mode_orders):
    network = stem_tensor
    for step_index in range(STEPS):
        group_start = (root_devices[step_index] // 4 * 4).astype(jnp.int32)
        leaf_group = lax.dynamic_slice_in_dim(leaves, group_start, 4, 0)[:, step_index]
        pair_low = complex_product(leaf_group[0], leaf_group[1]).astype(jnp.bfloat16)
        pair_high = complex_product(leaf_group[2], leaf_group[3]).astype(jnp.bfloat16)
        branch = complex_product(pair_low, pair_high)
        ordered = jnp.take(branch, column_source(mode_orders[step_index], BRANCH), axis=2)
        network = complex_product(network, ordered, lax.Precision.HIGHEST)
        if step_index % 2 == 0:
            stem_view = network.reshape(2, N_WIDE, N_NARROW, ROWS_DEV, N_NARROW, BRANCH // N_NARROW)
            network = jnp.swapaxes(stem_view, 2, 4).reshape(network.shape)
    return network
```

```python
import jax
import jax.numpy as jnp
from jax import lax
from jax.sharding import PartitionSpec as P

GROUP = 4


def from_partner(value, axis, mask):
    return lax.ppermute(value, axis, [(i, i ^ mask) for i in range(lax.axis_size(axis))])


def complex_product(a, b):
    def dot(x, y):
        return jnp.dot(x, y, preferred_element_type=jnp.float32)

    real_part = dot(a[0], b[0]) - dot(a[1], b[1])
    imag_part = dot(a[0], b[1]) + dot(a[1], b[0])
    return jnp.stack([real_part, imag_part])


def column_source(order_row, branch_width):
    column = jnp.arange(branch_width, dtype=jnp.int32)
    modes = jnp.arange(order_row.shape[0], dtype=jnp.int32)
    bits = jnp.right_shift(column[:, None], modes[None, :]) & 1
    return jnp.sum(bits * jnp.left_shift(jnp.int32(1), order_row)[None, :], axis=1)


def both_cores(half, axis):
    other = from_partner(half, "narrow", 1)
    core = lax.axis_index("narrow")
    low = jnp.where(core == 0, half, other)
    high = jnp.where(core == 0, other, half)
    return jnp.concatenate([low, high], axis=axis)


def local(stem_tensor, leaves, root_devices, mode_orders):
    width = stem_tensor.shape[2]
    rows = stem_tensor.shape[1]
    half = width // 2
    core = lax.axis_index("narrow")
    wide = lax.axis_index("wide")
    groups = lax.axis_size("wide") // GROUP
    member = wide % GROUP
    y = member % 2
    z = member // 2
    group = wide // GROUP
    bf16 = jnp.bfloat16

    by_parity = leaves[0].reshape(2, 2, 2, width, width)
    mine = lax.dynamic_index_in_dim(by_parity, y, 1, False)
    theirs = lax.dynamic_index_in_dim(by_parity, 1 - y, 1, False)
    sent = lax.dynamic_slice_in_dim(theirs, core * half, half, 2)
    got = both_cores(from_partner(sent, "wide", 1), 2)
    left = jnp.where(y == 0, mine, got)
    right = jnp.where(y == 0, got, mine)
    left = lax.dynamic_slice_in_dim(left, core * half, half, 2)
    pairs = jnp.stack([complex_product(left[i], right[i]).astype(bf16) for i in range(2)])
    own = lax.dynamic_index_in_dim(pairs, z, 0, False)
    away = lax.dynamic_index_in_dim(pairs, 1 - z, 0, False)
    came = from_partner(away, "wide", 2)
    low = jnp.where(z == 0, own, came)
    high = jnp.where(z == 0, came, own)
    source = column_source(lax.dynamic_index_in_dim(mode_orders, member, 0, False), width)
    chosen = (jnp.arange(width, dtype=jnp.int32)[:, None] == source[None, :]).astype(bf16)
    high = jnp.dot(high, chosen, preferred_element_type=jnp.float32).astype(bf16)
    branch = complex_product(low, both_cores(high, 1)).astype(bf16)
    root_group = lax.dynamic_index_in_dim(root_devices, member, 0, False) // GROUP
    step = 1
    while step < groups:
        other = from_partner(branch, "wide", GROUP * step)
        branch = jnp.where((root_group & step) == (group & step), branch, other)
        step *= 2
    first, second = branch[:, : half // 2], branch[:, half // 2 :]
    first_y = from_partner(first, "wide", 1)
    second_z = from_partner(second, "wide", 2)
    pair_y = jnp.stack([first, first_y])
    pair_z = jnp.stack([second, second_z])
    over_z = from_partner(pair_y, "wide", 2)
    over_y = from_partner(pair_z, "wide", 1)
    all_first = jnp.concatenate([pair_y, over_z])
    all_second = jnp.stack([second, over_y[0], second_z, over_y[1]])
    gathered = jnp.concatenate([all_first, all_second], axis=2)
    gathered = both_cores(gathered, 2)

    network = stem_tensor.astype(bf16)
    for k in range(4):
        ordered = lax.dynamic_index_in_dim(gathered, member ^ k, 0, False)
        network = complex_product(network, ordered)
        if k < 3:
            network = network.astype(bf16)
        if k % 2 == 0:
            keep = lax.dynamic_slice_in_dim(network, core * half, half, 2)
            give = lax.dynamic_slice_in_dim(network, (1 - core) * half, half, 2)
            take = from_partner(give, "narrow", 1)
            network = jnp.concatenate(
                [jnp.where(core == 0, keep, take), jnp.where(core == 0, take, keep)], axis=2
            )
    return network


def solution(mesh):
    stem_spec = P(None, ("cuts", "wide", "narrow"), None)
    return jax.shard_map(
        local,
        mesh=mesh,
        in_specs=(stem_spec, P(("cuts", "wide"), None, None, None, None), P(), P()),
        out_specs=stem_spec,
        check_vma=False,
    )
```

```python
import functools

import jax
import jax.numpy as jnp
from jax import lax
from jax.experimental import pallas as pl
from jax.experimental.pallas import tpu as pltpu
from jax.sharding import PartitionSpec as P

GROUP = 4
CHUNKS = 4
TILE = 128
BF16 = jnp.bfloat16
F32 = jnp.float32


def dot(x, y):
    return jnp.dot(x, y, preferred_element_type=F32)


def complex_product(ar, ai, br, bi):
    return dot(ar, br) - dot(ai, bi), dot(ar, bi) + dot(ai, br)


def remote(src, dst, send_sem, recv_sem, device):
    return pltpu.make_async_remote_copy(
        src_ref=src,
        dst_ref=dst,
        send_sem=send_sem,
        recv_sem=recv_sem,
        device_id=device,
        device_id_type=pl.DeviceIdType.MESH,
    )


def kernel(
    rounds, roots, orders, stem_in, leaves_in, out,
    leaf, pair, away, high, chosen, held, crossed, branches, stem, net1, net2, net3, swap,
    local_sem, leaf_s, leaf_r, fwd_s, fwd_r, pair_s, pair_r, high_s, high_r,
    cross_s, cross_r, z_s, z_r, y_s, y_r, core_s, core_r, swap_s, swap_r,
):
    width = stem.shape[2]
    rows = stem.shape[1]
    half = width // 2
    part = half // CHUNKS
    core = lax.axis_index("narrow")
    wide = lax.axis_index("wide")
    member = wide % GROUP
    y = member % 2
    z = member // 2
    other = {"narrow": 1 - core}
    over_y = {"wide": wide + 1 - 2 * y}
    over_z = {"wide": wide + 2 - 4 * z}
    bits = [(wide // (GROUP << r)) % 2 for r in range(rounds)]
    over_group = [{"wide": wide + (GROUP << r) * (1 - 2 * bits[r])} for r in range(rounds)]

    barrier = pltpu.get_barrier_semaphore()
    for peer in [other, over_y, over_z] + over_group:
        pl.semaphore_signal(barrier, inc=1, device_id=peer, device_id_type=pl.DeviceIdType.MESH)
    own_rows = pl.ds(pl.multiple_of(core * half, half), half)
    own_copies = [
        pltpu.make_async_copy(leaves_in.at[0, 2 * s + y], leaf.at[s, y], local_sem.at[s])
        for s in range(2)
    ]
    stem_copy = pltpu.make_async_copy(stem_in, stem, local_sem.at[2])
    pl.semaphore_wait(barrier, 3 + rounds)

    phases = [1 - z, z]
    leaf_copies = []
    for i, s in enumerate(phases):
        copy = remote(
            leaves_in.at[0, 2 * s + 1 - y, :, own_rows],
            leaf.at[s, y, :, own_rows],
            leaf_s.at[i], leaf_r.at[i], over_y,
        )
        copy.start()
        leaf_copies.append(copy)
    for copy in own_copies:
        copy.start()
    stem_copy.start()

    def choose(i, carry):
        column = lax.broadcasted_iota(jnp.int32, (TILE, width), 1)
        source = jnp.zeros((TILE, width), jnp.int32)
        for b in range(orders.shape[1]):
            weight = jnp.left_shift(jnp.int32(1), orders[member, b])
            source = source + (jnp.right_shift(column, b) & 1) * weight
        row = lax.broadcasted_iota(jnp.int32, (TILE, width), 0) + i * TILE
        at = pl.ds(pl.multiple_of(i * TILE, TILE), TILE)
        chosen[at] = jnp.where(row == source, 1.0, 0.0).astype(F32).astype(BF16)
        return carry

    lax.fori_loop(0, width // TILE, choose, 0)
    for copy in own_copies:
        copy.wait()

    pair_copy = remote(away, pair.at[z], pair_s, pair_r, over_z)
    for i, s in enumerate(phases):
        leaf_copies[i].wait_recv()
        forward = remote(
            leaf.at[s, 1 - y, :, own_rows], leaf.at[s, 1 - y, :, own_rows],
            fwd_s.at[i], fwd_r.at[i], other,
        )
        forward.start()
        forward.wait()

        def pair_tile(t, carry, s=s, i=i):
            source = pl.ds(pl.multiple_of(core * half + t * TILE, TILE), TILE)
            at = pl.ds(pl.multiple_of(t * TILE, TILE), TILE)
            real, imag = complex_product(
                leaf[s, 0, 0, source], leaf[s, 0, 1, source], leaf[s, 1, 0], leaf[s, 1, 1]
            )
            target = away if i == 0 else pair.at[z]
            target[0, at] = real.astype(BF16)
            target[1, at] = imag.astype(BF16)
            return carry

        lax.fori_loop(0, half // TILE, pair_tile, 0)
        if i == 0:
            pair_copy.start()
    pair_copy.wait_recv()

    def high_tile(t, carry):
        source = pl.ds(pl.multiple_of(t * TILE, TILE), TILE)
        at = pl.ds(pl.multiple_of(core * half + t * TILE, TILE), TILE)
        for c in range(2):
            high[c, at] = dot(pair[1, c, source], chosen[...]).astype(BF16)
        return carry

    lax.fori_loop(0, half // TILE, high_tile, 0)
    high_copy = remote(high.at[:, own_rows], high.at[:, own_rows], high_s, high_r, other)
    high_copy.start()
    high_copy.wait()

    def rows_of(c):
        return pl.ds(pl.multiple_of(core * half + c * part, part), part)

    def cross_copy(r, c):
        return remote(held.at[r, c], crossed.at[r, c], cross_s.at[r, c], cross_r.at[r, c], over_group[r])

    def place(origin, c):
        return branches.at[origin, :, rows_of(c)]

    origins = [member, member + 2 - 4 * z, member + 1 - 2 * y, GROUP - 1 - member]

    def z_copy(c):
        return remote(place(origins[0], c), place(origins[0], c), z_s.at[c], z_r.at[c], over_z)

    def y_copy(i, c):
        return remote(place(origins[i], c), place(origins[i], c), y_s.at[i, c], y_r.at[i, c], over_y)

    def core_copy(i, c):
        return remote(place(origins[i], c), place(origins[i], c), core_s.at[i, c], core_r.at[i, c], other)

    for c in range(CHUNKS):
        at = pl.ds(c * part, part)
        real, imag = complex_product(pair[0, 0, at], pair[0, 1, at], high[0], high[1])
        if rounds:
            held[0, c, 0] = real.astype(BF16)
            held[0, c, 1] = imag.astype(BF16)
            cross_copy(0, c).start()
        else:
            branches[member, 0, rows_of(c)] = real.astype(BF16)
            branches[member, 1, rows_of(c)] = imag.astype(BF16)

    for r in range(rounds):
        root_bit = (roots[member] // (GROUP << r)) % 2
        for c in range(CHUNKS):
            cross_copy(r, c).wait_recv()
            for p in range(2):
                here = held[r, c, p].astype(F32)
                there = crossed[r, c, p].astype(F32)
                same = jnp.full(here.shape, root_bit, jnp.int32) == bits[r]
                picked = jnp.where(same, here, there).astype(BF16)
                if r + 1 < rounds:
                    held[r + 1, c, p] = picked
                else:
                    branches[member, p, rows_of(c)] = picked
            if r + 1 < rounds:
                cross_copy(r + 1, c).start()
            else:
                z_copy(c).start()
                y_copy(0, c).start()
                core_copy(0, c).start()
                if c > 0:
                    z_copy(c - 1).wait_recv()
                    y_copy(1, c - 1).start()
                    core_copy(1, c - 1).start()
                    y_copy(0, c - 1).wait_recv()
                    core_copy(2, c - 1).start()
                if c > 1:
                    y_copy(1, c - 2).wait_recv()
                    core_copy(3, c - 2).start()
    if not rounds:
        for c in range(CHUNKS):
            z_copy(c).start()
            y_copy(0, c).start()
            core_copy(0, c).start()
    for c in range(0 if not rounds else CHUNKS - 1, CHUNKS):
        z_copy(c).wait_recv()
        y_copy(1, c).start()
        core_copy(1, c).start()
        y_copy(0, c).wait_recv()
        core_copy(2, c).start()
    for c in range(0 if not rounds else CHUNKS - 2, CHUNKS):
        y_copy(1, c).wait_recv()
        core_copy(3, c).start()
    stem_copy.wait()
    for c in range(CHUNKS):
        for i in range(4):
            core_copy(i, c).wait_recv()

    def columns(block):
        return pl.ds(pl.multiple_of(block * half, half), half)

    def swapped(step, index, read, target):
        copy = remote(swap.at[index], target.at[core], swap_s.at[index], swap_r.at[index], other)
        for keep in range(2):
            block = core if keep else 1 - core

            def tile(t, carry, keep=keep, block=block):
                at = pl.ds(pl.multiple_of(t * TILE, TILE), TILE)
                nr, ni = read(at)
                real, imag = complex_product(
                    nr, ni, branches[step, 0, :, columns(block)], branches[step, 1, :, columns(block)]
                )
                place = target.at[core] if keep else swap.at[index]
                place[0, at] = real.astype(BF16)
                place[1, at] = imag.astype(BF16)
                return carry

            lax.fori_loop(0, rows // TILE, tile, 0)
            if not keep:
                copy.start()
        copy.wait()

    def plain(step, source, target):
        def tile(t, carry):
            at = pl.ds(pl.multiple_of(t * TILE, TILE), TILE)
            real = jnp.zeros((TILE, width), F32)
            imag = jnp.zeros((TILE, width), F32)
            for block in range(2):
                inner = pl.ds(block * half, half)
                dr, di = complex_product(
                    source[block, 0, at], source[block, 1, at],
                    branches[step, 0, inner], branches[step, 1, inner],
                )
                real, imag = real + dr, imag + di
            target[0, at] = real.astype(target.dtype)
            target[1, at] = imag.astype(target.dtype)
            return carry

        lax.fori_loop(0, rows // TILE, tile, 0)

    swapped(0, 0, lambda at: (stem[0, at].astype(BF16), stem[1, at].astype(BF16)), net1)
    plain(1, net1, net2)
    swapped(2, 1, lambda at: (net2[0, at], net2[1, at]), net3)
    plain(3, net3, out)

    for copy in leaf_copies:
        copy.wait_send()
    pair_copy.wait_send()
    for c in range(CHUNKS):
        for r in range(rounds):
            cross_copy(r, c).wait_send()
        z_copy(c).wait_send()
        for i in range(2):
            y_copy(i, c).wait_send()
        for i in range(4):
            core_copy(i, c).wait_send()


def local(stem_tensor, leaves, root_devices, mode_orders):
    _, rows, width = stem_tensor.shape
    half = width // 2
    part = half // CHUNKS
    groups = lax.axis_size("wide") // GROUP
    rounds = groups.bit_length() - 1
    vmem = pltpu.VMEM
    dma = pltpu.SemaphoreType.DMA
    return pl.pallas_call(
        functools.partial(kernel, rounds),
        out_shape=jax.ShapeDtypeStruct(stem_tensor.shape, F32),
        in_specs=[pl.BlockSpec(memory_space=pltpu.SMEM)] * 2
        + [pl.BlockSpec(memory_space=pl.ANY)] * 2,
        out_specs=pl.BlockSpec(memory_space=pltpu.VMEM),
        scratch_shapes=[
            vmem((2, 2, 2, width, width), BF16),
            vmem((2, 2, half, width), BF16),
            vmem((2, half, width), BF16),
            vmem((2, width, width), BF16),
            vmem((width, width), BF16),
            vmem((max(rounds, 1), CHUNKS, 2, part, width), BF16),
            vmem((max(rounds, 1), CHUNKS, 2, part, width), BF16),
            vmem((GROUP, 2, width, width), BF16),
            vmem((2, rows, width), F32),
            vmem((2, 2, rows, half), BF16),
            vmem((2, rows, width), BF16),
            vmem((2, 2, rows, half), BF16),
            vmem((2, 2, rows, half), BF16),
            dma((3,)),
            dma((2,)), dma((2,)), dma((2,)), dma((2,)),
            dma, dma, dma, dma,
            dma((max(rounds, 1), CHUNKS)), dma((max(rounds, 1), CHUNKS)),
            dma((CHUNKS,)), dma((CHUNKS,)),
            dma((2, CHUNKS)), dma((2, CHUNKS)),
            dma((4, CHUNKS)), dma((4, CHUNKS)),
            dma((2,)), dma((2,)),
        ],
        compiler_params=pltpu.CompilerParams(collective_id=0, has_side_effects=True),
    )(root_devices, mode_orders, stem_tensor, leaves)


def solution(mesh):
    stem_spec = P(None, ("cuts", "wide", "narrow"), None)
    return jax.shard_map(
        local,
        mesh=mesh,
        in_specs=(stem_spec, P(("cuts", "wide"), None, None, None, None), P(), P()),
        out_specs=stem_spec,
        check_vma=False,
    )
```

```python
import functools

import jax
import jax.numpy as jnp
from jax import lax
from jax.experimental import pallas as pl
from jax.experimental.pallas import tpu as pltpu
from jax.sharding import PartitionSpec as P

GROUP = 4
CHUNKS = 8
FLIGHT = 2
TILE = 128
BF16 = jnp.bfloat16
F32 = jnp.float32


def dot(x, y):
    return jnp.dot(x, y, preferred_element_type=F32)


def complex_product(ar, ai, br, bi):
    left = jnp.concatenate([ar, ai], axis=1)
    return (
        dot(left, jnp.concatenate([br, -bi], axis=0)),
        dot(left, jnp.concatenate([bi, br], axis=0)),
    )


def remote(src, dst, send_sem, recv_sem, device):
    return pltpu.make_async_remote_copy(
        src_ref=src,
        dst_ref=dst,
        send_sem=send_sem,
        recv_sem=recv_sem,
        device_id=device,
        device_id_type=pl.DeviceIdType.MESH,
    )


def kernel(
    rounds, roots, orders, stem_in, leaves_in, net_out, last_out,
    leaf, pair, away, high, chosen, held, crossed, branches, stem, net1, net2, net3, swap,
    local_sem, leaf_s, leaf_r, fwd_s, fwd_r, pair_s, pair_r, high_s, high_r,
    cross_s, cross_r, z_s, z_r, y_s, y_r, core_s, core_r, swap_s, swap_r,
):
    width = stem.shape[2]
    rows = stem.shape[1]
    half = width // 2
    part = half // CHUNKS
    core = lax.axis_index("narrow")
    wide = lax.axis_index("wide")
    member = wide % GROUP
    y = member % 2
    z = member // 2
    other = {"narrow": 1 - core}
    over_y = {"wide": wide + 1 - 2 * y}
    over_z = {"wide": wide + 2 - 4 * z}
    bits = [(wide // (GROUP << r)) % 2 for r in range(rounds)]
    over_group = [{"wide": wide + (GROUP << r) * (1 - 2 * bits[r])} for r in range(rounds)]

    barrier = pltpu.get_barrier_semaphore()
    for peer in [other, over_y, over_z] + over_group:
        pl.semaphore_signal(barrier, inc=1, device_id=peer, device_id_type=pl.DeviceIdType.MESH)
    own_rows = pl.ds(pl.multiple_of(core * half, half), half)
    own_copies = [
        pltpu.make_async_copy(leaves_in.at[0, 2 * s + y], leaf.at[s, y], local_sem.at[s])
        for s in range(2)
    ]
    stem_copy = pltpu.make_async_copy(stem_in, stem, local_sem.at[2])
    pl.semaphore_wait(barrier, 3 + rounds)

    phases = [1 - z, z]
    leaf_copies = []
    for i, s in enumerate(phases):
        copy = remote(
            leaves_in.at[0, 2 * s + 1 - y, :, own_rows],
            leaf.at[s, y, :, own_rows],
            leaf_s.at[i], leaf_r.at[i], over_y,
        )
        leaf_copies.append(copy)
    leaf_copies[0].start()
    for copy in own_copies:
        copy.start()
    stem_copy.start()

    def choose(i, carry):
        column = lax.broadcasted_iota(jnp.int32, (TILE, width), 1)
        source = jnp.zeros((TILE, width), jnp.int32)
        for b in range(orders.shape[1]):
            weight = jnp.left_shift(jnp.int32(1), orders[member, b])
            source = source + (jnp.right_shift(column, b) & 1) * weight
        row = lax.broadcasted_iota(jnp.int32, (TILE, width), 0) + i * TILE
        at = pl.ds(pl.multiple_of(i * TILE, TILE), TILE)
        chosen[at] = jnp.where(row == source, 1.0, 0.0).astype(F32).astype(BF16)
        return carry

    lax.fori_loop(0, width // TILE, choose, 0)
    for copy in own_copies:
        copy.wait()

    pair_copy = remote(away, pair.at[z], pair_s, pair_r, over_z)
    leaf_copies[0].wait_send()
    leaf_copies[1].start()
    for i, s in enumerate(phases):
        leaf_copies[i].wait_recv()
        forward = remote(
            leaf.at[s, 1 - y, :, own_rows], leaf.at[s, 1 - y, :, own_rows],
            fwd_s.at[i], fwd_r.at[i], other,
        )
        forward.start()
        forward.wait()

        def pair_tile(t, carry, s=s, i=i):
            at = pl.ds(pl.multiple_of(t * half, half), half)
            real, imag = complex_product(
                leaf[s, 0, 0, own_rows], leaf[s, 0, 1, own_rows],
                leaf[s, 1, 0, :, at], leaf[s, 1, 1, :, at],
            )
            target = away if i == 0 else pair.at[z]
            target[0, :, at] = real.astype(BF16)
            target[1, :, at] = imag.astype(BF16)
            return carry

        lax.fori_loop(0, width // half, pair_tile, 0)
        if i == 0:
            pair_copy.start()
    pair_copy.wait_recv()

    def high_tile(t, carry):
        at = pl.ds(pl.multiple_of(t * half, half), half)
        for c in range(2):
            high[c, own_rows, at] = dot(pair[1, c], chosen[:, at]).astype(BF16)
        return carry

    lax.fori_loop(0, width // half, high_tile, 0)
    high_copy = remote(high.at[:, own_rows], high.at[:, own_rows], high_s, high_r, other)
    high_copy.start()
    high_copy.wait()

    def rows_of(c):
        return pl.ds(pl.multiple_of(core * half + c * part, part), part)

    def cross_copy(r, c):
        return remote(held.at[r, c], crossed.at[r, c], cross_s.at[r, c], cross_r.at[r, c], over_group[r])

    def place(origin, c):
        return branches.at[origin, :, rows_of(c)]

    origins = [member, member + 2 - 4 * z, member + 1 - 2 * y, GROUP - 1 - member]

    def z_copy(c):
        return remote(place(origins[0], c), place(origins[0], c), z_s.at[c], z_r.at[c], over_z)

    def y_copy(i, c):
        return remote(place(origins[i], c), place(origins[i], c), y_s.at[i, c], y_r.at[i, c], over_y)

    def core_copy(i, c):
        return remote(place(origins[i], c), place(origins[i], c), core_s.at[i, c], core_r.at[i, c], other)

    def spread(c):
        z_copy(c).start()
        y_copy(0, c).start()
        core_copy(0, c).start()

    def select(r, c):
        cross_copy(r, c).wait_recv()
        cross_copy(r, c).wait_send()
        if c + FLIGHT < CHUNKS:
            cross_copy(r, c + FLIGHT).start()
        root_bit = (roots[member] // (GROUP << r)) % 2
        for p in range(2):
            here = held[r, c, p].astype(F32)
            there = crossed[r, c, p].astype(F32)
            same = jnp.full(here.shape, root_bit, jnp.int32) == bits[r]
            picked = jnp.where(same, here, there).astype(BF16)
            if r + 1 < rounds:
                held[r + 1, c, p] = picked
            else:
                branches[member, p, rows_of(c)] = picked
        if r + 1 < rounds:
            if c < FLIGHT:
                cross_copy(r + 1, c).start()
        else:
            spread(c)

    def on_z(c):
        z_copy(c).wait_recv()
        y_copy(1, c).start()
        core_copy(1, c).start()

    def on_y(i, c):
        y_copy(i, c).wait_recv()
        core_copy(2 + i, c).start()

    for c in range(CHUNKS):
        at = pl.ds(c * part, part)
        real, imag = complex_product(pair[0, 0, at], pair[0, 1, at], high[0], high[1])
        if rounds:
            held[0, c, 0] = real.astype(BF16)
            held[0, c, 1] = imag.astype(BF16)
            if c < FLIGHT:
                cross_copy(0, c).start()
        else:
            branches[member, 0, rows_of(c)] = real.astype(BF16)
            branches[member, 1, rows_of(c)] = imag.astype(BF16)
            spread(c)

    for r in range(rounds - 1):
        for c in range(CHUNKS):
            select(r, c)
    for c in range(CHUNKS + 2):
        if rounds and c < CHUNKS:
            select(rounds - 1, c)
        if 1 <= c <= CHUNKS:
            on_z(c - 1)
            on_y(0, c - 1)
        if c >= 2:
            on_y(1, c - 2)
    stem_copy.wait()
    for c in range(CHUNKS):
        for i in range(4):
            core_copy(i, c).wait_recv()
    last_copy = pltpu.make_async_copy(branches.at[GROUP - 1], last_out, local_sem.at[3])
    last_copy.start()

    def columns(block):
        return pl.ds(pl.multiple_of(block * half, half), half)

    def swapped(step, index, read, target):
        copy = remote(swap.at[index], target.at[core], swap_s.at[index], swap_r.at[index], other)
        for keep in range(2):
            block = core if keep else 1 - core

            def tile(t, carry, keep=keep, block=block):
                at = pl.ds(pl.multiple_of(t * half, half), half)
                nr, ni = read(at)
                real, imag = complex_product(
                    nr, ni, branches[step, 0, :, columns(block)], branches[step, 1, :, columns(block)]
                )
                place = target.at[core] if keep else swap.at[index]
                place[0, at] = real.astype(BF16)
                place[1, at] = imag.astype(BF16)
                return carry

            lax.fori_loop(0, rows // half, tile, 0)
            if not keep:
                copy.start()
        copy.wait()

    def plain(step, source, target):
        for block in range(width // half):
            across = pl.ds(block * half, half)

            def tile(t, carry, across=across):
                at = pl.ds(pl.multiple_of(t * half, half), half)
                real, imag = complex_product(
                    jnp.concatenate([source[0, 0, at], source[1, 0, at]], axis=1),
                    jnp.concatenate([source[0, 1, at], source[1, 1, at]], axis=1),
                    branches[step, 0, :, across], branches[step, 1, :, across],
                )
                target[0, at, across] = real.astype(target.dtype)
                target[1, at, across] = imag.astype(target.dtype)
                return carry

            lax.fori_loop(0, rows // half, tile, 0)

    swapped(0, 0, lambda at: (stem[0, at].astype(BF16), stem[1, at].astype(BF16)), net1)
    plain(1, net1, net2)
    swapped(2, 1, lambda at: (net2[0, at], net2[1, at]), net3)
    net_copy = pltpu.make_async_copy(net3, net_out, local_sem.at[4])
    net_copy.start()
    net_copy.wait()
    last_copy.wait()

    leaf_copies[1].wait_send()
    pair_copy.wait_send()
    for c in range(CHUNKS):
        z_copy(c).wait_send()
        for i in range(2):
            y_copy(i, c).wait_send()
        for i in range(4):
            core_copy(i, c).wait_send()


def finish(net, branch, out):
    half = net.shape[3]
    for block in range(branch.shape[2] // half):
        across = pl.ds(block * half, half)
        real, imag = complex_product(
            jnp.concatenate([net[0, 0], net[1, 0]], axis=1),
            jnp.concatenate([net[0, 1], net[1, 1]], axis=1),
            branch[0, :, across], branch[1, :, across],
        )
        out[0, :, across] = real
        out[1, :, across] = imag


def local(stem_tensor, leaves, root_devices, mode_orders):
    _, rows, width = stem_tensor.shape
    half = width // 2
    part = half // CHUNKS
    groups = lax.axis_size("wide") // GROUP
    rounds = groups.bit_length() - 1
    vmem = pltpu.VMEM
    dma = pltpu.SemaphoreType.DMA
    network, last = pl.pallas_call(
        functools.partial(kernel, rounds),
        out_shape=(
            jax.ShapeDtypeStruct((2, 2, rows, half), BF16),
            jax.ShapeDtypeStruct((2, width, width), BF16),
        ),
        in_specs=[pl.BlockSpec(memory_space=pltpu.SMEM)] * 2
        + [pl.BlockSpec(memory_space=pl.ANY)] * 2,
        out_specs=[pl.BlockSpec(memory_space=pl.ANY)] * 2,
        scratch_shapes=[
            vmem((2, 2, 2, width, width), BF16),
            vmem((2, 2, half, width), BF16),
            vmem((2, half, width), BF16),
            vmem((2, width, width), BF16),
            vmem((width, width), BF16),
            vmem((max(rounds, 1), CHUNKS, 2, part, width), BF16),
            vmem((max(rounds, 1), CHUNKS, 2, part, width), BF16),
            vmem((GROUP, 2, width, width), BF16),
            vmem((2, rows, width), F32),
            vmem((2, 2, rows, half), BF16),
            vmem((2, rows, width), BF16),
            vmem((2, 2, rows, half), BF16),
            vmem((2, 2, rows, half), BF16),
            dma((5,)),
            dma((2,)), dma((2,)), dma((2,)), dma((2,)),
            dma, dma, dma, dma,
            dma((max(rounds, 1), CHUNKS)), dma((max(rounds, 1), CHUNKS)),
            dma((CHUNKS,)), dma((CHUNKS,)),
            dma((2, CHUNKS)), dma((2, CHUNKS)),
            dma((4, CHUNKS)), dma((4, CHUNKS)),
            dma((2,)), dma((2,)),
        ],
        compiler_params=pltpu.CompilerParams(collective_id=0, has_side_effects=True),
    )(root_devices, mode_orders, stem_tensor, leaves)
    return pl.pallas_call(
        finish,
        grid=(rows // half,),
        out_shape=jax.ShapeDtypeStruct(stem_tensor.shape, F32),
        in_specs=[
            pl.BlockSpec((2, 2, half, half), lambda i: (0, 0, i, 0)),
            pl.BlockSpec((2, width, width), lambda i: (0, 0, 0)),
        ],
        out_specs=pl.BlockSpec((2, half, width), lambda i: (0, i, 0)),
    )(network, last)


def solution(mesh):
    stem_spec = P(None, ("cuts", "wide", "narrow"), None)
    return jax.shard_map(
        local,
        mesh=mesh,
        in_specs=(stem_spec, P(("cuts", "wide"), None, None, None, None), P(), P()),
        out_specs=stem_spec,
        check_vma=False,
    )
```
